32 devices in a mesh: seq: 8 (over z, y), tp: 4 (over x, core).
Axes of the slice: x: 2, y: 2, z: 4, core: 2. Of those that a mesh axis runs over, the one named last changes fastest.
Arguments:
- query_act: bfloat16 [2048, 4096], P('seq', 'tp'), may hold values from -6 to 6
- key_act: bfloat16 [2048, 1024], P('seq', 'tp'), may hold values from -6 to 6
- value_act: bfloat16 [2048, 1024], P('seq', 'tp'), may hold values from -6 to 6
- attn_out: bfloat16 [2048, 4096], P('seq', 'tp'), may hold values from -6 to 6
- out_grad: bfloat16 [2048, 4096], P('seq', 'tp'), may hold values from -6 to 6
- log_sum: float32 [32, 2048], P('tp', 'seq'), as said below
- positions: int32 [2048], P('seq'), may hold values from 0 to 2047, as said below
- w_query: bfloat16 [4096, 4096], P(None, 'tp'), may hold values from -0.09375 to 0.09375
- w_key: bfloat16 [4096, 1024], P(None, 'tp'), may hold values from -0.09375 to 0.09375
- w_value: bfloat16 [4096, 1024], P(None, 'tp'), may hold values from -0.09375 to 0.09375
Outputs:
- input_grad: bfloat16 [2048, 4096], P('seq', 'tp')
The draws below stay inside these ranges and needn't reach their ends.
Inputs may be any that keep to these rules, and one draw needn't show every extreme that they name: The rows of one index of seq are two runs of 128 consecutive positions, each run starting at a multiple of 128; all rows together hold every position 0 to 2047 once. log_sum[h, t] lies within 0.5 of log(positions[t] + 1) + 0.5.
All inputs are finite; a program needn't handle non-finite values.
Results may differ from the reference program's by a relative error of at most 0.0057.
Values may be sent and summed in bfloat16 or wider, within the bound.
A program may use at most 64 MiB of HBM per device.

```python
import jax
import jax.numpy as jnp
from jax import lax

D = 4096
HEADS = 32
KV_HEADS = 8
HEAD_DIM = 128
TOK_DEV = 256
TOKENS = 2048


def shared_places(key):
    count = 2 * (TOKENS // TOK_DEV)
    half_rows = TOK_DEV // 2
    order = jax.random.permutation(jax.random.fold_in(key, 71), count)
    return (order[:, None] * half_rows + jnp.arange(half_rows)[None, :]).reshape(-1).astype(jnp.int32)


def draw_positions(key, part):
    return shared_places(key)


def draw_log_sum(key, part):
    places = shared_places(key).astype(jnp.float32)
    noise = jax.random.uniform(jax.random.fold_in(key, 23), (HEADS, TOKENS), jnp.float32, -0.25, 0.25)
    return jnp.log(places + 1.0)[None, :] + 0.5 + noise


def block_scale(rng, dims, split, least, top_value):
    gain, own = 1.0, jax.random.fold_in(rng, 6)
    for axis_at, blocks in split:
        draws = jnp.exp(jax.random.uniform(jax.random.fold_in(own, axis_at), (blocks,), jnp.float32, least / len(split), top_value / len(split)))
        gain = gain * jnp.repeat(draws, dims[axis_at] // blocks).reshape([-1 if axis == axis_at else 1 for axis in range(len(dims))])
    return gain


def scatter_about(key, extent, width, bound, split=(), held_as=jnp.bfloat16):
    entries = jax.random.normal(key, extent, jnp.float32) * width
    if len(split) > 0:
        entries = block_scale(key, extent, split, -0.22, 0.18) * entries
    return jnp.clip(entries, min=-bound, max=bound).astype(held_as)


def setup_inputs(seed: int = 0) -> dict:
    key_list = jax.random.split(jax.random.key(seed), 11)
    query_act = scatter_about(key_list[0], (TOKENS, HEADS * HEAD_DIM), 1.0, 6.0, ((0, 8), (1, 4)))
    key_act = scatter_about(key_list[1], (TOKENS, KV_HEADS * HEAD_DIM), 1.0, 6.0, ((0, 8), (1, 4)))
    value_act = scatter_about(key_list[2], (TOKENS, KV_HEADS * HEAD_DIM), 1.0, 6.0, ((0, 8), (1, 4)))
    attn_out = scatter_about(key_list[3], (TOKENS, HEADS * HEAD_DIM), 0.5, 6.0, ((0, 8), (1, 4)))
    out_grad = scatter_about(key_list[4], (TOKENS, HEADS * HEAD_DIM), 1.0, 6.0, ((0, 8), (1, 4)))
    log_sum = draw_log_sum(jax.random.fold_in(key_list[10], 71), 0)
    positions = draw_positions(jax.random.fold_in(key_list[10], 71), 0)
    w_query = scatter_about(key_list[7], (D, HEADS * HEAD_DIM), D ** -0.5, 0.09375, ((1, 4),))
    w_key = scatter_about(key_list[8], (D, KV_HEADS * HEAD_DIM), D ** -0.5, 0.09375, ((1, 4),))
    w_value = scatter_about(key_list[9], (D, KV_HEADS * HEAD_DIM), D ** -0.5, 0.09375, ((1, 4),))
    return {"query_act": query_act, "key_act": key_act, "value_act": value_act, "attn_out": attn_out, "out_grad": out_grad, "log_sum": log_sum, "positions": positions, "w_query": w_query, "w_key": w_key, "w_value": w_value}


def rotate_back(grads, places):
    half_dim = grads.shape[-1] // 2
    freqs = 500000.0 ** (-(jnp.arange(half_dim, dtype=jnp.float32) * 2.0 / grads.shape[-1]))
    angles = places.astype(jnp.float32)[:, None] * freqs[None, :]
    cosine = jnp.cos(angles)[:, None, :]
    sine = jnp.sin(angles)[:, None, :]
    first = grads[..., :half_dim]
    second = grads[..., half_dim:]
    return jnp.concatenate([first * cosine + second * sine, second * cosine - first * sine], axis=-1)


def reference(query_act, key_act, value_act, attn_out, out_grad, log_sum, positions, w_query, w_key, w_value):
    tokens = query_act.shape[0]
    repeat = HEADS // KV_HEADS
    scale = HEAD_DIM ** -0.5
    query_heads = query_act.reshape(tokens, KV_HEADS, repeat, HEAD_DIM).transpose(1, 0, 2, 3)
    dout_heads = out_grad.reshape(tokens, KV_HEADS, repeat, HEAD_DIM).transpose(1, 0, 2, 3)
    output_heads = attn_out.reshape(tokens, KV_HEADS, repeat, HEAD_DIM).transpose(1, 0, 2, 3)
    deltas = jnp.sum(dout_heads.astype(jnp.float32) * output_heads.astype(jnp.float32), -1)
    lse_heads = log_sum.reshape(KV_HEADS, repeat, tokens)
    key_heads = key_act.reshape(tokens, KV_HEADS, HEAD_DIM).transpose(1, 0, 2)
    value_heads = value_act.reshape(tokens, KV_HEADS, HEAD_DIM).transpose(1, 0, 2)
    blocks = tokens // TOK_DEV

    def one_group(operands):
        query_group, dout_group, delta_group, lse_group, key_group, value_group = operands
        query_float = query_group.astype(jnp.float32)
        dout_float = dout_group.astype(jnp.float32)

        def one_block(dq_total, block_index):
            start = (block_index * TOK_DEV).astype(jnp.int32)
            key_block = lax.dynamic_slice_in_dim(key_group, start, TOK_DEV, 0).astype(jnp.float32)
            value_block = lax.dynamic_slice_in_dim(value_group, start, TOK_DEV, 0).astype(jnp.float32)
            key_places = lax.dynamic_slice_in_dim(positions, start, TOK_DEV, 0)
            scores = jnp.einsum('qrd,kd->rqk', query_float, key_block) * scale
            visible = key_places[None, :] <= positions[:, None]
            probs = jnp.where(visible[None], jnp.exp(scores - lse_group[:, :, None]), 0.0)
            probs_low = lax.optimization_barrier(probs.astype(jnp.bfloat16)).astype(jnp.float32)
            value_grad = jnp.einsum('rqk,qrd->kd', probs_low, dout_float)
            prob_grad = jnp.einsum('qrd,kd->rqk', dout_float, value_block)
            score_grad = probs * (prob_grad - delta_group.T[:, :, None]) * scale
            score_low = lax.optimization_barrier(score_grad.astype(jnp.bfloat16)).astype(jnp.float32)
            dq_total = dq_total + jnp.einsum('rqk,kd->qrd', score_low, key_block)
            key_grad = jnp.einsum('rqk,qrd->kd', score_low, query_float)
            return dq_total, (key_grad, value_grad)

        start_dq = jnp.zeros((tokens, repeat, HEAD_DIM), jnp.float32)
        dq_total, (key_parts, value_parts) = lax.scan(one_block, start_dq, jnp.arange(blocks, dtype=jnp.int32))
        return dq_total, key_parts.reshape(tokens, HEAD_DIM), value_parts.reshape(tokens, HEAD_DIM)

    dq_all, dk_all, dv_all = lax.map(one_group, (query_heads, dout_heads, deltas, lse_heads, key_heads, value_heads))
    dq_all = dq_all.transpose(1, 0, 2, 3).reshape(tokens, HEADS, HEAD_DIM)
    dk_all = dk_all.transpose(1, 0, 2)
    dv_all = dv_all.transpose(1, 0, 2)
    query_grad = rotate_back(dq_all, positions).reshape(tokens, HEADS * HEAD_DIM).astype(jnp.bfloat16)
    key_grad = rotate_back(dk_all, positions).reshape(tokens, KV_HEADS * HEAD_DIM).astype(jnp.bfloat16)
    value_grad = dv_all.reshape(tokens, KV_HEADS * HEAD_DIM).astype(jnp.bfloat16)
    total = jnp.dot(query_grad, w_query.T, preferred_element_type=jnp.float32)
    total = total + jnp.dot(key_grad, w_key.T, preferred_element_type=jnp.float32)
    total = total + jnp.dot(value_grad, w_value.T, preferred_element_type=jnp.float32)
    return total.astype(jnp.bfloat16)
```

```python
import functools
import math

import jax
import jax.numpy as jnp
import numpy as np
from jax import lax
from jax.experimental import pallas as pl
from jax.experimental.pallas import tpu as pltpu
from jax.sharding import PartitionSpec as P

HEADS = 32
KV_HEADS = 8
HEAD_DIM = 128
MESH = pl.DeviceIdType.MESH
F32 = jnp.float32
BF16 = jnp.bfloat16
PIECE = 256
VMEM_LIMIT = 58 * 1024 * 1024


def ring_place(index, n):
    return jnp.where(index % 2 == 0, index // 2, n - 1 - index // 2)


def ring_index(place, n):
    return jnp.where(place < n // 2, 2 * place, 2 * (n - 1 - place) + 1)


def rotate(grad, cosine, sine):
    half = grad.shape[0] // 2
    first, second = grad[:half], grad[half:]
    return jnp.concatenate([first * cosine + second * sine, second * cosine - first * sine], axis=0)


def kernel(
    n,
    tp,
    groups,
    repeat,
    q_hbm,
    do_hbm,
    o_hbm,
    k_hbm,
    v_hbm,
    log_sum_ref,
    qpos_ref,
    freq_ref,
    wq_hbm,
    wk_hbm,
    wv_hbm,
    out_hbm,
    q_ref,
    do_ref,
    o_ref,
    dq_ref,
    dk_ref,
    dv_ref,
    wq_ref,
    wk_ref,
    wv_ref,
    lse_ref,
    delta_ref,
    pos_ref,
    terms,
    core_out,
    core_in,
    chip_out,
    chip_in,
    kv_buf,
    acc_out,
    acc_in,
    part,
    own,
    dq_acc,
    out_ref,
    kv_send,
    kv_recv,
    acc_send,
    acc_recv,
    load_sem,
    in_sem,
    kvin_sem,
    out_sem,
    core_send,
    core_recv,
    chip_send,
    chip_recv,
):
    rows, width = q_ref.shape
    half = rows // 2
    dim = width // (groups * repeat)
    scale = dim ** (-0.5)
    log2e = math.log2(math.e)
    place = ring_place(lax.axis_index("seq"), n)
    after = ring_index(lax.rem(place + 1, n), n)
    before = ring_index(lax.rem(place + n - 1, n), n)
    targets = [after if g % 2 == 0 else before for g in range(groups)]

    barrier = pltpu.get_barrier_semaphore()
    for other in (after, before):
        pl.semaphore_signal(barrier, inc=1, device_id={"seq": other}, device_id_type=MESH)
    rank = lax.axis_index("tp")
    chips = tp // 2
    chip, core = rank // 2, lax.rem(rank, 2)
    partner = 2 * chip + 1 - core
    chip_order = [lax.rem(chip + 1 + j, chips) for j in range(chips)]
    peers = [2 * chip_order[j] + core for j in range(chips - 1)]
    for other in [partner] + peers:
        pl.semaphore_signal(barrier, inc=1, device_id={"tp": other}, device_id_type=MESH)

    kv_loads = []
    for g in range(groups):
        cut = pl.ds(g * dim, dim)
        for i, src in enumerate((k_hbm, v_hbm)):
            kv_loads.append(
                pltpu.make_async_copy(
                    src.at[:, cut], kv_buf.at[g, 0, pl.ds(i * rows, rows), :], kvin_sem.at[g, i]
                )
            )
            kv_loads[-1].start()
    in_loads = [
        pltpu.make_async_copy(src, dst, in_sem.at[i])
        for i, (src, dst) in enumerate(((q_hbm, q_ref), (do_hbm, do_ref), (o_hbm, o_ref)))
    ]
    for load in in_loads:
        load.start()
    loads = [
        pltpu.make_async_copy(src, dst, load_sem.at[i])
        for i, (src, dst) in enumerate(((wq_hbm, wq_ref), (wk_hbm, wk_ref), (wv_hbm, wv_ref)))
    ]
    for load in loads:
        load.start()

    qpos = qpos_ref[...].astype(F32)
    pos_ref[...] = qpos
    first_tag = jnp.broadcast_to(qpos[:, 0:1] * (1.0 / half), (8, dim))
    second_tag = jnp.broadcast_to(qpos[:, half : half + 1] * (1.0 / half), (8, dim))
    tags = jnp.concatenate([first_tag, second_tag], axis=0).astype(BF16)
    for g in range(groups):
        kv_buf[g, 0, 2 * rows : 2 * rows + 16, :] = tags

    def kv_copy(g, step):
        return pltpu.make_async_remote_copy(
            src_ref=kv_buf.at[g, step],
            dst_ref=kv_buf.at[g, step + 1],
            send_sem=kv_send.at[g, step],
            recv_sem=kv_recv.at[g, step + 1],
            device_id={"seq": targets[g]},
            device_id_type=MESH,
        )

    def acc_copy(g, step):
        return pltpu.make_async_remote_copy(
            src_ref=acc_out.at[g, step],
            dst_ref=acc_in.at[g, step + 1],
            send_sem=acc_send.at[g, step],
            recv_sem=acc_recv.at[g, step + 1],
            device_id={"seq": targets[g]},
            device_id_type=MESH,
        )

    def kv_arrival(g, step):
        return pltpu.make_async_remote_copy(
            src_ref=kv_buf.at[g, step],
            dst_ref=kv_buf.at[g, step],
            send_sem=kv_send.at[g, step],
            recv_sem=kv_recv.at[g, step],
            device_id={"seq": targets[g]},
            device_id_type=MESH,
        )

    def acc_arrival(g, step):
        return pltpu.make_async_remote_copy(
            src_ref=acc_in.at[g, step],
            dst_ref=acc_in.at[g, step],
            send_sem=acc_send.at[g, 0],
            recv_sem=acc_recv.at[g, step],
            device_id={"seq": targets[g]},
            device_id_type=MESH,
        )

    for load in kv_loads:
        load.wait()
    pl.semaphore_wait(barrier, 2 + chips)
    for g in range(groups):
        kv_copy(g, 0).start()

    lse_ref[...] = log_sum_ref[...] * log2e
    for load in in_loads:
        load.wait()
    for h in range(groups * repeat):
        cut = slice(h * dim, (h + 1) * dim)
        both = do_ref[:, cut].astype(F32) * o_ref[:, cut].astype(F32)
        delta_ref[h : h + 1, :] = jnp.sum(both.T, axis=0, keepdims=True)

    def attend(g, block, result, first):
        k = block[0:rows, :]
        v = block[rows : 2 * rows, :]
        tags = block[2 * rows : 2 * rows + 16, :].astype(F32)
        low = jnp.concatenate([tags[0:1, :] * half] * (rows // dim), axis=1)
        high = jnp.concatenate([tags[8:9, :] * half] * (rows // dim), axis=1)
        if first:
            gap = pos_ref[...] - lax.broadcasted_iota(jnp.int32, (half, rows), 0).astype(F32)
            seen = jnp.concatenate([gap >= low, gap >= high], axis=0)
        else:
            low = jnp.where(pos_ref[...] >= low, 0.0, 1e30)
            high = jnp.where(pos_ref[...] >= high, 0.0, 1e30)
        kt = k.T
        dk = jnp.zeros((rows, dim), F32)
        dv = jnp.zeros((rows, dim), F32)
        for r in range(repeat):
            h = g * repeat + r
            q = q_ref[:, h * dim : (h + 1) * dim]
            do = do_ref[:, h * dim : (h + 1) * dim]
            nt = (((1,), (1,)), ((), ()))
            s = lax.dot_general(k, q, nt, preferred_element_type=F32) * (scale * log2e)
            lse = lse_ref[h : h + 1, :]
            if first:
                p = jnp.where(seen, jnp.exp2(s - lse), 0.0)
            else:
                p = jnp.concatenate(
                    [jnp.exp2(s[:half] - (lse + low)), jnp.exp2(s[half:] - (lse + high))], axis=0
                )
            dv += jnp.dot(p.astype(BF16), do, preferred_element_type=F32)
            dp = lax.dot_general(v, do, nt, preferred_element_type=F32)
            ds = (p * (dp - delta_ref[h : h + 1, :])).astype(BF16)
            dk += jnp.dot(ds, q, preferred_element_type=F32)
            dqt = jnp.dot(kt, ds, preferred_element_type=F32)
            if first:
                dq_acc[h] = dqt
            else:
                dq_acc[h] += dqt
        result[g, 0] = dk * scale
        result[g, 1] = dv

    for g in range(groups):
        attend(g, kv_buf.at[g, 0], own, True)

    def turn(step, carry):
        for g in range(groups):
            kv_arrival(g, step).wait_recv()

            @pl.when(step < n - 1)
            def _():
                kv_copy(g, step).start()

        for g in range(groups):
            attend(g, kv_buf.at[g, step], part, False)

            @pl.when(step == 1)
            def _():
                acc_out[g, step] = part[g].astype(BF16)

            @pl.when(step > 1)
            def _():
                acc_arrival(g, step).wait_recv()
                acc_out[g, step] = (part[g] + acc_in[g, step].astype(F32)).astype(BF16)

            acc_copy(g, step).start()
        return carry

    lax.fori_loop(1, n, turn, 0)

    angles = freq_ref[...] * pos_ref[...]
    cosine = jnp.cos(angles)
    sine = jnp.sin(angles)
    for h in range(groups * repeat):
        dq_ref[:, h * dim : (h + 1) * dim] = rotate(dq_acc[h] * scale, cosine, sine).T.astype(BF16)
    cols = out_hbm.shape[1]
    pieces = max(1, cols // PIECE)
    wide = cols // pieces

    def span(block, piece):
        return pl.ds(pl.multiple_of(block * cols + piece * wide, wide), wide)

    for load in loads:
        load.wait()
    far = [2 * chip_order[j] + 1 - core for j in range(chips)]
    near = [2 * chip_order[j] + core for j in range(chips)]

    def query_terms(piece, carry):
        for j in range(chips):
            for i, block in enumerate((far[j], near[j])):
                terms[2 * j + i, piece] = project(dq_ref[...], wq_ref[span(block, piece), :])
        return carry

    lax.fori_loop(0, pieces, query_terms, 0)
    for g in range(groups):
        acc_arrival(g, n).wait_recv()
        total = own[g] + acc_in[g, n].astype(F32)
        dk_ref[:, g * dim : (g + 1) * dim] = rotate(total[0].T, cosine, sine).T.astype(BF16)
        dv_ref[:, g * dim : (g + 1) * dim] = total[1].astype(BF16)

    def full_terms(slot, block, piece):
        total = terms[slot, piece] + project(dk_ref[...], wk_ref[span(block, piece), :])
        return total + project(dv_ref[...], wv_ref[span(block, piece), :])

    def core_copy(j, piece):
        return pltpu.make_async_remote_copy(
            src_ref=core_out.at[j, piece],
            dst_ref=core_in.at[j, piece],
            send_sem=core_send.at[j, piece],
            recv_sem=core_recv.at[j, piece],
            device_id={"tp": partner},
            device_id_type=MESH,
        )

    def chip_copy(j, piece):
        return pltpu.make_async_remote_copy(
            src_ref=chip_out.at[j, piece],
            dst_ref=chip_in.at[j, piece],
            send_sem=chip_send.at[j, piece],
            recv_sem=chip_recv.at[j, piece],
            device_id={"tp": peers[j]},
            device_id_type=MESH,
        )

    def relay(j, piece):
        core_copy(j, piece).wait_recv()
        mine = terms[2 * j + 1, piece] + core_in[j, piece].astype(F32)
        if j < chips - 1:
            chip_out[j, piece] = mine.astype(BF16)
            chip_copy(j, piece).start()
        else:
            terms[2 * j + 1, piece] = mine

    for j in range(chips):
        for piece in range(pieces):
            core_out[j, piece] = full_terms(2 * j, far[j], piece).astype(BF16)
            core_copy(j, piece).start()
            terms[2 * j + 1, piece] = full_terms(2 * j + 1, near[j], piece)
            if piece > 0:
                relay(j, piece - 1)
        relay(j, pieces - 1)

    def out_copy(piece):
        cut = pl.ds(piece * wide, wide)
        return pltpu.make_async_copy(out_ref.at[:, cut], out_hbm.at[:, cut], out_sem.at[piece])

    for piece in range(pieces):
        total = terms[2 * chips - 1, piece]
        for j in range(chips - 1):
            chip_copy(j, piece).wait_recv()
            total = total + chip_in[j, piece].astype(F32)
        out_ref[:, piece * wide : (piece + 1) * wide] = total.astype(BF16)
        out_copy(piece).start()
    for piece in range(pieces):
        for j in range(chips):
            core_copy(j, piece).wait_send()
        for j in range(chips - 1):
            chip_copy(j, piece).wait_send()

    def drain(step, carry):
        for g in range(groups):
            kv_copy(g, step).wait_send()

            @pl.when(step > 0)
            def _():
                acc_copy(g, step).wait_send()

        return carry

    lax.fori_loop(0, n - 1, drain, 0)
    for g in range(groups):
        acc_copy(g, n - 1).wait_send()
    for piece in range(pieces):
        out_copy(piece).wait()


def project(grads, weight):
    return lax.dot_general(grads, weight, (((1,), (1,)), ((), ())), preferred_element_type=F32)


def shards(
    n, tp, query_act, key_act, value_act, attn_out, out_grad, log_sum, positions, w_query, w_key, w_value
):
    rows, width = query_act.shape
    dim = HEAD_DIM
    repeat = HEADS // KV_HEADS
    groups = key_act.shape[1] // dim
    heads = groups * repeat
    half = rows // 2
    model = w_query.shape[0]
    cols = model // tp
    chips = tp // 2
    freqs = np.float32(500000.0) ** (-(np.arange(dim // 2, dtype=np.float32) * 2.0 / dim))
    pieces = max(1, cols // PIECE)
    wide = cols // pieces
    vmem = pl.BlockSpec(memory_space=pltpu.VMEM)
    hbm = pl.BlockSpec(memory_space=pl.ANY)
    return pl.pallas_call(
        functools.partial(kernel, n, tp, groups, repeat),
        out_shape=jax.ShapeDtypeStruct((rows, cols), BF16),
        in_specs=[hbm] * 5 + [vmem] * 3 + [hbm] * 3,
        out_specs=hbm,
        scratch_shapes=[
            pltpu.VMEM((rows, width), BF16),
            pltpu.VMEM((rows, width), BF16),
            pltpu.VMEM((rows, width), BF16),
            pltpu.VMEM((rows, width), BF16),
            pltpu.VMEM((rows, groups * dim), BF16),
            pltpu.VMEM((rows, groups * dim), BF16),
            pltpu.VMEM(w_query.shape, BF16),
            pltpu.VMEM(w_key.shape, BF16),
            pltpu.VMEM(w_value.shape, BF16),
            pltpu.VMEM((heads, rows), F32),
            pltpu.VMEM((heads, rows), F32),
            pltpu.VMEM((1, rows), F32),
            pltpu.VMEM((tp, pieces, rows, wide), F32),
            pltpu.VMEM((chips, pieces, rows, wide), BF16),
            pltpu.VMEM((chips, pieces, rows, wide), BF16),
            pltpu.VMEM((chips - 1, pieces, rows, wide), BF16),
            pltpu.VMEM((chips - 1, pieces, rows, wide), BF16),
            pltpu.VMEM((groups, n, 2 * rows + 16, dim), BF16),
            pltpu.VMEM((groups, n, 2, rows, dim), BF16),
            pltpu.VMEM((groups, n + 1, 2, rows, dim), BF16),
            pltpu.VMEM((groups, 2, rows, dim), F32),
            pltpu.VMEM((groups, 2, rows, dim), F32),
            pltpu.VMEM((heads, dim, rows), F32),
            pltpu.VMEM((rows, cols), BF16),
            pltpu.SemaphoreType.DMA((groups, n + 1)),
            pltpu.SemaphoreType.DMA((groups, n + 1)),
            pltpu.SemaphoreType.DMA((groups, n + 1)),
            pltpu.SemaphoreType.DMA((groups, n + 1)),
            pltpu.SemaphoreType.DMA((3,)),
            pltpu.SemaphoreType.DMA((3,)),
            pltpu.SemaphoreType.DMA((groups, 2)),
            pltpu.SemaphoreType.DMA((pieces,)),
            pltpu.SemaphoreType.DMA((chips, pieces)),
            pltpu.SemaphoreType.DMA((chips, pieces)),
            pltpu.SemaphoreType.DMA((chips - 1, pieces)),
            pltpu.SemaphoreType.DMA((chips - 1, pieces)),
        ],
        compiler_params=pltpu.CompilerParams(
            collective_id=0, has_side_effects=True, vmem_limit_bytes=VMEM_LIMIT
        ),
    )(
        query_act,
        out_grad,
        attn_out,
        key_act,
        value_act,
        log_sum,
        positions[None, :],
        jnp.asarray(freqs)[:, None],
        w_query,
        w_key,
        w_value,
    )


def solution(mesh):
    return jax.shard_map(
        functools.partial(shards, mesh.shape["seq"], mesh.shape["tp"]),
        mesh=mesh,
        in_specs=(
            P("seq", "tp"),
            P("seq", "tp"),
            P("seq", "tp"),
            P("seq", "tp"),
            P("seq", "tp"),
            P("tp", "seq"),
            P("seq"),
            P(None, "tp"),
            P(None, "tp"),
            P(None, "tp"),
        ),
        out_specs=P("seq", "tp"),
        check_vma=False,
    )
```

```python
import functools
import math

import jax
import jax.numpy as jnp
import numpy as np
from jax import lax
from jax.experimental import pallas as pl
from jax.experimental.pallas import tpu as pltpu
from jax.sharding import PartitionSpec as P

HEADS = 32
KV_HEADS = 8
HEAD_DIM = 128
MESH = pl.DeviceIdType.MESH
F32 = jnp.float32
BF16 = jnp.bfloat16
PIECE = 256
VMEM_LIMIT = 58 * 1024 * 1024
OUT = pltpu.VMEM
ORDER = (
    ("take", 0, 0),
    ("take", 1, 1),
    ("take", 0, 1),
    ("work", 0, 0),
    ("give", 0, 1),
    ("take", 1, 0),
    ("work", 1, 0),
    ("give", 1, 0),
    ("give", 0, 0),
    ("give", 1, 1),
)


def ring_place(index, n):
    return jnp.where(index % 2 == 0, index // 2, n - 1 - index // 2)


def ring_index(place, n):
    return jnp.where(place < n // 2, 2 * place, 2 * (n - 1 - place) + 1)


def rotate(grad, cosine, sine):
    half = grad.shape[0] // 2
    first, second = grad[:half], grad[half:]
    return jnp.concatenate([first * cosine + second * sine, second * cosine - first * sine], axis=0)


def kernel(
    n,
    tp,
    groups,
    repeat,
    q_hbm,
    do_hbm,
    o_hbm,
    k_hbm,
    v_hbm,
    log_sum_ref,
    qpos_ref,
    freq_ref,
    wq_hbm,
    wk_hbm,
    wv_hbm,
    out_ref,
    q_ref,
    do_ref,
    o_ref,
    dq_ref,
    dk_ref,
    dv_ref,
    wq_ref,
    wk_ref,
    wv_ref,
    lse_ref,
    delta_ref,
    pos_ref,
    terms,
    core_out,
    core_in,
    chip_out,
    chip_in,
    kv_buf,
    acc_out,
    acc_in,
    part,
    own,
    dq_acc,
    kv_send,
    kv_recv,
    acc_send,
    acc_recv,
    load_sem,
    in_sem,
    kvin_sem,
    core_send,
    core_recv,
    chip_send,
    chip_recv,
):
    rows, width = q_ref.shape
    half = rows // 2
    dim = width // (groups * repeat)
    scale = dim ** (-0.5)
    log2e = math.log2(math.e)
    place = ring_place(lax.axis_index("seq"), n)
    after = ring_index(lax.rem(place + 1, n), n)
    before = ring_index(lax.rem(place + n - 1, n), n)
    targets = [after if g % 2 == 0 else before for g in range(groups)]

    barrier = pltpu.get_barrier_semaphore()
    for other in (after, before):
        pl.semaphore_signal(barrier, inc=1, device_id={"seq": other}, device_id_type=MESH)
    rank = lax.axis_index("tp")
    chips = tp // 2
    chip, core = rank // 2, lax.rem(rank, 2)
    partner = 2 * chip + 1 - core
    chip_order = [lax.rem(chip + 1 + j, chips) for j in range(chips)]
    peers = [2 * chip_order[j] + core for j in range(chips - 1)]
    for other in [partner] + peers:
        pl.semaphore_signal(barrier, inc=1, device_id={"tp": other}, device_id_type=MESH)

    kv_loads = []
    for g in range(groups):
        cut = pl.ds(g * dim, dim)
        for i, src in enumerate((k_hbm, v_hbm)):
            kv_loads.append(
                pltpu.make_async_copy(
                    src.at[:, cut], kv_buf.at[g, 0, pl.ds(i * rows, rows), :], kvin_sem.at[g, i]
                )
            )
            kv_loads[-1].start()
    in_loads = [
        pltpu.make_async_copy(src, dst, in_sem.at[i])
        for i, (src, dst) in enumerate(((q_hbm, q_ref), (do_hbm, do_ref), (o_hbm, o_ref)))
    ]
    for load in in_loads:
        load.start()
    loads = [
        pltpu.make_async_copy(src, dst, load_sem.at[i])
        for i, (src, dst) in enumerate(((wq_hbm, wq_ref), (wk_hbm, wk_ref), (wv_hbm, wv_ref)))
    ]

    qpos = qpos_ref[...].astype(F32)
    pos_ref[...] = qpos
    first_tag = jnp.broadcast_to(qpos[:, 0:1] * (1.0 / half), (8, dim))
    second_tag = jnp.broadcast_to(qpos[:, half : half + 1] * (1.0 / half), (8, dim))
    tags = jnp.concatenate([first_tag, second_tag], axis=0).astype(BF16)
    for g in range(groups):
        kv_buf[g, 0, 2 * rows : 2 * rows + 16, :] = tags

    def slot(g, step, i):
        return kv_buf.at[g, step, pl.ds(i * rows, rows + 16 * i), :]

    def kv_copy(g, step, i):
        return pltpu.make_async_remote_copy(
            src_ref=slot(g, step, i),
            dst_ref=slot(g, step + 1, i),
            send_sem=kv_send.at[g, i, step],
            recv_sem=kv_recv.at[g, i, step + 1],
            device_id={"seq": targets[g]},
            device_id_type=MESH,
        )

    def acc_copy(g, step, i):
        return pltpu.make_async_remote_copy(
            src_ref=acc_out.at[g, step, i],
            dst_ref=acc_in.at[g, step + 1, i],
            send_sem=acc_send.at[g, i, step],
            recv_sem=acc_recv.at[g, i, step + 1],
            device_id={"seq": targets[g]},
            device_id_type=MESH,
        )

    def kv_arrival(g, step, i):
        return pltpu.make_async_remote_copy(
            src_ref=slot(g, step, i),
            dst_ref=slot(g, step, i),
            send_sem=kv_send.at[g, i, step],
            recv_sem=kv_recv.at[g, i, step],
            device_id={"seq": targets[g]},
            device_id_type=MESH,
        )

    def acc_arrival(g, step, i):
        return pltpu.make_async_remote_copy(
            src_ref=acc_in.at[g, step, i],
            dst_ref=acc_in.at[g, step, i],
            send_sem=acc_send.at[g, i, 0],
            recv_sem=acc_recv.at[g, i, step],
            device_id={"seq": targets[g]},
            device_id_type=MESH,
        )

    for load in kv_loads:
        load.wait()
    pl.semaphore_wait(barrier, 2 + chips)
    for i in range(2):
        for g in range(groups):
            kv_copy(g, 0, i).start()
    for load in loads:
        load.start()

    lse_ref[...] = log_sum_ref[...] * log2e
    for load in in_loads:
        load.wait()
    for h in range(groups * repeat):
        cut = slice(h * dim, (h + 1) * dim)
        both = do_ref[:, cut].astype(F32) * o_ref[:, cut].astype(F32)
        delta_ref[h : h + 1, :] = jnp.sum(both.T, axis=0, keepdims=True)

    def attend(g, block, result, first):
        k = block[0:rows, :]
        v = block[rows : 2 * rows, :]
        tags = block[2 * rows : 2 * rows + 16, :].astype(F32)
        low = jnp.concatenate([tags[0:1, :] * half] * (rows // dim), axis=1)
        high = jnp.concatenate([tags[8:9, :] * half] * (rows // dim), axis=1)
        if first:
            gap = pos_ref[...] - lax.broadcasted_iota(jnp.int32, (half, rows), 0).astype(F32)
            seen = jnp.concatenate([gap >= low, gap >= high], axis=0)
        else:
            low = jnp.where(pos_ref[...] >= low, 0.0, 1e30)
            high = jnp.where(pos_ref[...] >= high, 0.0, 1e30)
        kt = k.T
        dk = jnp.zeros((rows, dim), F32)
        dv = jnp.zeros((rows, dim), F32)
        for r in range(repeat):
            h = g * repeat + r
            q = q_ref[:, h * dim : (h + 1) * dim]
            do = do_ref[:, h * dim : (h + 1) * dim]
            nt = (((1,), (1,)), ((), ()))
            s = lax.dot_general(k, q, nt, preferred_element_type=F32) * (scale * log2e)
            lse = lse_ref[h : h + 1, :]
            if first:
                p = jnp.where(seen, jnp.exp2(s - lse), 0.0)
            else:
                p = jnp.concatenate(
                    [jnp.exp2(s[:half] - (lse + low)), jnp.exp2(s[half:] - (lse + high))], axis=0
                )
            dv += jnp.dot(p.astype(BF16), do, preferred_element_type=F32)
            dp = lax.dot_general(v, do, nt, preferred_element_type=F32)
            ds = (p * (dp - delta_ref[h : h + 1, :])).astype(BF16)
            dk += jnp.dot(ds, q, preferred_element_type=F32)
            dqt = jnp.dot(kt, ds, preferred_element_type=F32)
            if first:
                dq_acc[h] = dqt
            else:
                dq_acc[h] += dqt
        result[g, 0] = dk * scale
        result[g, 1] = dv

    for g in range(groups):
        attend(g, kv_buf.at[g, 0], own, True)

    def take(g, i, step):
        kv_arrival(g, step, i).wait_recv()

        @pl.when(step < n - 1)
        def _():
            kv_copy(g, step, i).start()

    def give(g, i, step):
        @pl.when(step == 1)
        def _():
            acc_out[g, step, i] = part[g, i].astype(BF16)

        @pl.when(step > 1)
        def _():
            acc_arrival(g, step, i).wait_recv()
            acc_out[g, step, i] = (part[g, i] + acc_in[g, step, i].astype(F32)).astype(BF16)

        acc_copy(g, step, i).start()

    def turn(step, carry):
        for act, g, i in ORDER:
            if g >= groups:
                continue
            if act == "take":
                take(g, i, step)
            elif act == "work":
                attend(g, kv_buf.at[g, step], part, False)
            else:
                give(g, i, step)
        return carry

    lax.fori_loop(1, n, turn, 0)

    angles = freq_ref[...] * pos_ref[...]
    cosine = jnp.cos(angles)
    sine = jnp.sin(angles)
    for h in range(groups * repeat):
        dq_ref[:, h * dim : (h + 1) * dim] = rotate(dq_acc[h] * scale, cosine, sine).T.astype(BF16)
    cols = out_ref.shape[1]
    pieces = max(1, cols // PIECE)
    wide = cols // pieces

    def span(block, piece):
        return pl.ds(pl.multiple_of(block * cols + piece * wide, wide), wide)

    for load in loads:
        load.wait()
    far = [2 * chip_order[j] + 1 - core for j in range(chips)]
    near = [2 * chip_order[j] + core for j in range(chips)]

    def query_terms(piece, carry):
        for j in range(chips):
            for i, block in enumerate((far[j], near[j])):
                terms[2 * j + i, piece] = project(dq_ref[...], wq_ref[span(block, piece), :])
        return carry

    lax.fori_loop(0, pieces, query_terms, 0)
    for g in range(groups):
        for i in range(2):
            acc_arrival(g, n, i).wait_recv()
        total = own[g] + acc_in[g, n].astype(F32)
        dk_ref[:, g * dim : (g + 1) * dim] = rotate(total[0].T, cosine, sine).T.astype(BF16)
        dv_ref[:, g * dim : (g + 1) * dim] = total[1].astype(BF16)

    def full_terms(slot, block, piece):
        total = terms[slot, piece] + project(dk_ref[...], wk_ref[span(block, piece), :])
        return total + project(dv_ref[...], wv_ref[span(block, piece), :])

    def core_copy(j, piece):
        return pltpu.make_async_remote_copy(
            src_ref=core_out.at[j, piece],
            dst_ref=core_in.at[j, piece],
            send_sem=core_send.at[j, piece],
            recv_sem=core_recv.at[j, piece],
            device_id={"tp": partner},
            device_id_type=MESH,
        )

    def chip_copy(j, piece):
        return pltpu.make_async_remote_copy(
            src_ref=chip_out.at[j, piece],
            dst_ref=chip_in.at[j, piece],
            send_sem=chip_send.at[j, piece],
            recv_sem=chip_recv.at[j, piece],
            device_id={"tp": peers[j]},
            device_id_type=MESH,
        )

    def relay(j, piece):
        core_copy(j, piece).wait_recv()
        mine = terms[2 * j + 1, piece] + core_in[j, piece].astype(F32)
        if j < chips - 1:
            chip_out[j, piece] = mine.astype(BF16)
            chip_copy(j, piece).start()
        else:
            terms[2 * j + 1, piece] = mine

    for j in range(chips):
        for piece in range(pieces):
            core_out[j, piece] = full_terms(2 * j, far[j], piece).astype(BF16)
            core_copy(j, piece).start()
        for piece in range(pieces):
            terms[2 * j + 1, piece] = full_terms(2 * j + 1, near[j], piece)
            relay(j, piece)

    for piece in range(pieces):
        total = terms[2 * chips - 1, piece]
        for j in range(chips - 1):
            chip_copy(j, piece).wait_recv()
            total = total + chip_in[j, piece].astype(F32)
        out_ref[:, piece * wide : (piece + 1) * wide] = total.astype(BF16)
    for piece in range(pieces):
        for j in range(chips):
            core_copy(j, piece).wait_send()
        for j in range(chips - 1):
            chip_copy(j, piece).wait_send()

    def drain(step, carry):
        for g in range(groups):
            for i in range(2):
                kv_copy(g, step, i).wait_send()

                @pl.when(step > 0)
                def _():
                    acc_copy(g, step, i).wait_send()

        return carry

    lax.fori_loop(0, n - 1, drain, 0)
    for g in range(groups):
        for i in range(2):
            acc_copy(g, n - 1, i).wait_send()


def project(grads, weight):
    return lax.dot_general(grads, weight, (((1,), (1,)), ((), ())), preferred_element_type=F32)


def shards(
    n, tp, query_act, key_act, value_act, attn_out, out_grad, log_sum, positions, w_query, w_key, w_value
):
    rows, width = query_act.shape
    dim = HEAD_DIM
    repeat = HEADS // KV_HEADS
    groups = key_act.shape[1] // dim
    heads = groups * repeat
    half = rows // 2
    model = w_query.shape[0]
    cols = model // tp
    chips = tp // 2
    freqs = np.float32(500000.0) ** (-(np.arange(dim // 2, dtype=np.float32) * 2.0 / dim))
    pieces = max(1, cols // PIECE)
    wide = cols // pieces
    vmem = pl.BlockSpec(memory_space=pltpu.VMEM)
    hbm = pl.BlockSpec(memory_space=pl.ANY)
    return pl.pallas_call(
        functools.partial(kernel, n, tp, groups, repeat),
        out_shape=OUT((rows, cols), BF16),
        in_specs=[hbm] * 5 + [vmem] * 3 + [hbm] * 3,
        out_specs=vmem,
        scratch_shapes=[
            pltpu.VMEM((rows, width), BF16),
            pltpu.VMEM((rows, width), BF16),
            pltpu.VMEM((rows, width), BF16),
            pltpu.VMEM((rows, width), BF16),
            pltpu.VMEM((rows, groups * dim), BF16),
            pltpu.VMEM((rows, groups * dim), BF16),
            pltpu.VMEM(w_query.shape, BF16),
            pltpu.VMEM(w_key.shape, BF16),
            pltpu.VMEM(w_value.shape, BF16),
            pltpu.VMEM((heads, rows), F32),
            pltpu.VMEM((heads, rows), F32),
            pltpu.VMEM((1, rows), F32),
            pltpu.VMEM((tp, pieces, rows, wide), F32),
            pltpu.VMEM((chips, pieces, rows, wide), BF16),
            pltpu.VMEM((chips, pieces, rows, wide), BF16),
            pltpu.VMEM((chips - 1, pieces, rows, wide), BF16),
            pltpu.VMEM((chips - 1, pieces, rows, wide), BF16),
            pltpu.VMEM((groups, n, 2 * rows + 16, dim), BF16),
            pltpu.VMEM((groups, n, 2, rows, dim), BF16),
            pltpu.VMEM((groups, n + 1, 2, rows, dim), BF16),
            pltpu.VMEM((groups, 2, rows, dim), F32),
            pltpu.VMEM((groups, 2, rows, dim), F32),
            pltpu.VMEM((heads, dim, rows), F32),
            pltpu.SemaphoreType.DMA((groups, 2, n + 1)),
            pltpu.SemaphoreType.DMA((groups, 2, n + 1)),
            pltpu.SemaphoreType.DMA((groups, 2, n + 1)),
            pltpu.SemaphoreType.DMA((groups, 2, n + 1)),
            pltpu.SemaphoreType.DMA((3,)),
            pltpu.SemaphoreType.DMA((3,)),
            pltpu.SemaphoreType.DMA((groups, 2)),
            pltpu.SemaphoreType.DMA((chips, pieces)),
            pltpu.SemaphoreType.DMA((chips, pieces)),
            pltpu.SemaphoreType.DMA((chips - 1, pieces)),
            pltpu.SemaphoreType.DMA((chips - 1, pieces)),
        ],
        compiler_params=pltpu.CompilerParams(
            collective_id=0, has_side_effects=True, vmem_limit_bytes=VMEM_LIMIT
        ),
    )(
        query_act,
        out_grad,
        attn_out,
        key_act,
        value_act,
        log_sum,
        positions[None, :],
        jnp.asarray(freqs)[:, None],
        w_query,
        w_key,
        w_value,
    )


def solution(mesh):
    return jax.shard_map(
        functools.partial(shards, mesh.shape["seq"], mesh.shape["tp"]),
        mesh=mesh,
        in_specs=(
            P("seq", "tp"),
            P("seq", "tp"),
            P("seq", "tp"),
            P("seq", "tp"),
            P("seq", "tp"),
            P("tp", "seq"),
            P("seq"),
            P(None, "tp"),
            P(None, "tp"),
            P(None, "tp"),
        ),
        out_specs=P("seq", "tp"),
        check_vma=False,
    )
```

```python
import functools
import math

import jax
import jax.numpy as jnp
import numpy as np
from jax import lax
from jax.experimental import pallas as pl
from jax.experimental.pallas import tpu as pltpu
from jax.sharding import PartitionSpec as P

HEADS = 32
KV_HEADS = 8
HEAD_DIM = 128
MESH = pl.DeviceIdType.MESH
F32 = jnp.float32
BF16 = jnp.bfloat16
PIECE = 512
VMEM_LIMIT = 58 * 1024 * 1024
OUT = pltpu.VMEM


def ring_place(index, n):
    return jnp.where(index % 2 == 0, index // 2, n - 1 - index // 2)


def ring_index(place, n):
    return jnp.where(place < n // 2, 2 * place, 2 * (n - 1 - place) + 1)


def rotate(grad, cosine, sine):
    half = grad.shape[0] // 2
    first, second = grad[:half], grad[half:]
    return jnp.concatenate([first * cosine + second * sine, second * cosine - first * sine], axis=0)


def kernel(
    n,
    tp,
    groups,
    repeat,
    q_hbm,
    do_hbm,
    o_hbm,
    k_hbm,
    v_hbm,
    log_sum_hbm,
    qpos_hbm,
    freq_hbm,
    wq_hbm,
    wk_hbm,
    wv_hbm,
    out_ref,
    q_ref,
    do_ref,
    o_ref,
    dq_ref,
    dk_ref,
    dv_ref,
    wq_ref,
    wk_ref,
    wv_ref,
    log_sum_ref,
    qpos_ref,
    freq_ref,
    lse_ref,
    delta_ref,
    pos_ref,
    cos_ref,
    sin_ref,
    terms,
    core_out,
    core_in,
    chip_out,
    chip_in,
    kv_buf,
    acc_out,
    acc_in,
    part,
    own,
    dq_acc,
    kv_send,
    kv_recv,
    acc_send,
    acc_recv,
    load_sem,
    in_sem,
    kvin_sem,
    small_sem,
    core_send,
    core_recv,
    chip_send,
    chip_recv,
):
    rows, width = q_ref.shape
    half = rows // 2
    dim = width // (groups * repeat)
    scale = dim ** (-0.5)
    log2e = math.log2(math.e)
    place = ring_place(lax.axis_index("seq"), n)
    after = ring_index(lax.rem(place + 1, n), n)
    before = ring_index(lax.rem(place + n - 1, n), n)
    targets = [after if g % 2 == 0 else before for g in range(groups)]

    barrier = pltpu.get_barrier_semaphore()
    for other in (after, before):
        pl.semaphore_signal(barrier, inc=1, device_id={"seq": other}, device_id_type=MESH)
    rank = lax.axis_index("tp")
    chips = tp // 2
    chip, core = rank // 2, lax.rem(rank, 2)
    partner = 2 * chip + 1 - core
    chip_order = [lax.rem(chip + 1 + j, chips) for j in range(chips)]
    peers = [2 * chip_order[j] + core for j in range(chips - 1)]
    for other in [partner] + peers:
        pl.semaphore_signal(barrier, inc=1, device_id={"tp": other}, device_id_type=MESH)

    small = [
        pltpu.make_async_copy(src, dst, small_sem.at[i])
        for i, (src, dst) in enumerate(
            ((qpos_hbm, qpos_ref), (log_sum_hbm, log_sum_ref), (freq_hbm, freq_ref))
        )
    ]
    small[0].start()
    kv_loads = []
    for g in range(groups):
        cut = pl.ds(g * dim, dim)
        for i, src in enumerate((k_hbm, v_hbm)):
            for r in range(2):
                load = pltpu.make_async_copy(
                    src.at[pl.ds(r * half, half), cut],
                    kv_buf.at[g, 0, r, pl.ds(i * half, half), :],
                    kvin_sem.at[g, i, r],
                )
                load.start()
                kv_loads.append(load)
    small[1].start()
    small[2].start()
    in_loads = [
        pltpu.make_async_copy(src, dst, in_sem.at[i])
        for i, (src, dst) in enumerate(((q_hbm, q_ref), (do_hbm, do_ref), (o_hbm, o_ref)))
    ]
    for load in in_loads:
        load.start()
    loads = [
        pltpu.make_async_copy(src, dst, load_sem.at[i])
        for i, (src, dst) in enumerate(((wq_hbm, wq_ref), (wk_hbm, wk_ref), (wv_hbm, wv_ref)))
    ]

    small[0].wait()
    qpos = qpos_ref[...].astype(F32)
    pos_ref[...] = qpos
    for r in range(2):
        tag = jnp.broadcast_to(qpos[:, r * half : r * half + 1] * (1.0 / half), (8, dim)).astype(BF16)
        for g in range(groups):
            kv_buf[g, 0, r, 2 * half : 2 * half + 8, :] = tag

    def kv_copy(g, step, i):
        return pltpu.make_async_remote_copy(
            src_ref=kv_buf.at[g, step, i],
            dst_ref=kv_buf.at[g, step + 1, i],
            send_sem=kv_send.at[g, i, step],
            recv_sem=kv_recv.at[g, i, step + 1],
            device_id={"seq": targets[g]},
            device_id_type=MESH,
        )

    def acc_copy(g, step, i):
        return pltpu.make_async_remote_copy(
            src_ref=acc_out.at[g, step, i],
            dst_ref=acc_in.at[g, step + 1, i],
            send_sem=acc_send.at[g, i, step],
            recv_sem=acc_recv.at[g, i, step + 1],
            device_id={"seq": targets[g]},
            device_id_type=MESH,
        )

    def kv_arrival(g, step, i):
        return pltpu.make_async_remote_copy(
            src_ref=kv_buf.at[g, step, i],
            dst_ref=kv_buf.at[g, step, i],
            send_sem=kv_send.at[g, i, step],
            recv_sem=kv_recv.at[g, i, step],
            device_id={"seq": targets[g]},
            device_id_type=MESH,
        )

    def acc_arrival(g, step, i):
        return pltpu.make_async_remote_copy(
            src_ref=acc_in.at[g, step, i],
            dst_ref=acc_in.at[g, step, i],
            send_sem=acc_send.at[g, i, 0],
            recv_sem=acc_recv.at[g, i, step],
            device_id={"seq": targets[g]},
            device_id_type=MESH,
        )

    for load in kv_loads:
        load.wait()
    pl.semaphore_wait(barrier, 2 + chips)
    for i in range(2):
        for g in range(groups):
            kv_copy(g, 0, i).start()
    for load in loads:
        load.start()

    small[1].wait()
    small[2].wait()
    lse_ref[...] = log_sum_ref[...] * log2e
    for load in in_loads:
        load.wait()
    for h in range(groups * repeat):
        cut = slice(h * dim, (h + 1) * dim)
        both = do_ref[:, cut].astype(F32) * o_ref[:, cut].astype(F32)
        delta_ref[h : h + 1, :] = jnp.sum(both.T, axis=0, keepdims=True)

    angles = freq_ref[:, 0:1] * pos_ref[...]
    cos_ref[...] = jnp.cos(angles)
    sin_ref[...] = jnp.sin(angles)

    def run(r):
        return slice(r * half, (r + 1) * half)

    def attend(g, r, block, result, first):
        k = block[0:half, :]
        v = block[half : 2 * half, :]
        tag = block[2 * half : 2 * half + 8, :].astype(F32)
        low = jnp.concatenate([tag[0:1, :] * half] * (rows // dim), axis=1)
        if first:
            gap = pos_ref[...] - lax.broadcasted_iota(jnp.int32, (half, rows), 0).astype(F32)
            seen = gap >= low
        else:
            hide = jnp.where(pos_ref[...] >= low, 0.0, 1e30)
        kt = k.T
        dk = jnp.zeros((half, dim), F32)
        dv = jnp.zeros((half, dim), F32)
        for c in range(repeat):
            h = g * repeat + c
            q = q_ref[:, h * dim : (h + 1) * dim]
            do = do_ref[:, h * dim : (h + 1) * dim]
            nt = (((1,), (1,)), ((), ()))
            s = lax.dot_general(k, q, nt, preferred_element_type=F32) * (scale * log2e)
            lse = lse_ref[h : h + 1, :]
            if first:
                p = jnp.where(seen, jnp.exp2(s - lse), 0.0)
            else:
                p = jnp.exp2(s - (lse + hide))
            dv += jnp.dot(p.astype(BF16), do, preferred_element_type=F32)
            dp = lax.dot_general(v, do, nt, preferred_element_type=F32)
            ds = (p * (dp - delta_ref[h : h + 1, :])).astype(BF16)
            dk += jnp.dot(ds, q, preferred_element_type=F32)
            dqt = jnp.dot(kt, ds, preferred_element_type=F32)
            if first and r == 0:
                dq_acc[h] = dqt
            else:
                dq_acc[h] += dqt
        result[g, 0, run(r), :] = dk * scale
        result[g, 1, run(r), :] = dv

    for r in range(2):
        for g in range(groups):
            attend(g, r, kv_buf.at[g, 0, r], own, True)

    def take(g, i, step):
        kv_arrival(g, step, i).wait_recv()

        @pl.when(step < n - 1)
        def _():
            kv_copy(g, step, i).start()

    def give(g, i, step):
        @pl.when(step == 1)
        def _():
            acc_out[g, step, i] = part[g, :, run(i), :].astype(BF16)

        @pl.when(step > 1)
        def _():
            acc_arrival(g, step, i).wait_recv()
            total = part[g, :, run(i), :] + acc_in[g, step, i].astype(F32)
            acc_out[g, step, i] = total.astype(BF16)

        acc_copy(g, step, i).start()

    def turn(step, carry):
        for r in range(2):
            for g in range(groups):
                take(g, r, step)
            for g in range(groups):
                attend(g, r, kv_buf.at[g, step, r], part, False)
            for g in range(groups):
                give(g, r, step)
        return carry

    lax.fori_loop(1, n, turn, 0)

    cosine = cos_ref[...]
    sine = sin_ref[...]
    for h in range(groups * repeat):
        dq_ref[:, h * dim : (h + 1) * dim] = rotate(dq_acc[h] * scale, cosine, sine).T.astype(BF16)
    cols = out_ref.shape[1]
    pieces = max(1, cols // PIECE)
    wide = cols // pieces

    def span(block, piece):
        return pl.ds(pl.multiple_of(block * cols + piece * wide, wide), wide)

    for load in loads:
        load.wait()
    far = [2 * chip_order[j] + 1 - core for j in range(chips)]
    near = [2 * chip_order[j] + core for j in range(chips)]

    def query_terms(slot, block, piece):
        both = project(dq_ref[...], wq_ref[span(block, piece), :])
        for r in range(2):
            terms[slot, r, piece] = both[run(r)]

    def finish_grads(r):
        for g in range(groups):
            acc_arrival(g, n, r).wait_recv()
            total = own[g, :, run(r), :] + acc_in[g, n, r].astype(F32)
            cut = slice(g * dim, (g + 1) * dim)
            turned = rotate(total[0].T, cosine[:, run(r)], sine[:, run(r)]).T
            dk_ref[run(r), cut] = turned.astype(BF16)
            dv_ref[run(r), cut] = total[1].astype(BF16)

    def full_terms(slot, block, r, piece):
        total = terms[slot, r, piece] + project(dk_ref[run(r), :], wk_ref[span(block, piece), :])
        return total + project(dv_ref[run(r), :], wv_ref[span(block, piece), :])

    def core_copy(j, r, piece):
        return pltpu.make_async_remote_copy(
            src_ref=core_out.at[j, r, piece],
            dst_ref=core_in.at[j, r, piece],
            send_sem=core_send.at[j, r, piece],
            recv_sem=core_recv.at[j, r, piece],
            device_id={"tp": partner},
            device_id_type=MESH,
        )

    def chip_copy(j, r, piece):
        return pltpu.make_async_remote_copy(
            src_ref=chip_out.at[j, r, piece],
            dst_ref=chip_in.at[j, r, piece],
            send_sem=chip_send.at[j, r, piece],
            recv_sem=chip_recv.at[j, r, piece],
            device_id={"tp": peers[j]},
            device_id_type=MESH,
        )

    def relay(j, r, piece):
        core_copy(j, r, piece).wait_recv()
        mine = terms[2 * j + 1, r, piece] + core_in[j, r, piece].astype(F32)
        if j < chips - 1:
            chip_out[j, r, piece] = mine.astype(BF16)
            chip_copy(j, r, piece).start()
        else:
            terms[2 * j + 1, r, piece] = mine

    def share(j, r):
        for piece in range(pieces):
            if r == 0:
                query_terms(2 * j, far[j], piece)
            core_out[j, r, piece] = full_terms(2 * j, far[j], r, piece).astype(BF16)
            core_copy(j, r, piece).start()
        for piece in range(pieces):
            if r == 0:
                query_terms(2 * j + 1, near[j], piece)
            terms[2 * j + 1, r, piece] = full_terms(2 * j + 1, near[j], r, piece)
            relay(j, r, piece)

    for r in range(2):
        finish_grads(r)
        for j in range(chips - 1):
            share(j, r)
    for r in range(2):
        share(chips - 1, r)

    for r in range(2):
        for piece in range(pieces):
            total = terms[2 * chips - 1, r, piece]
            for j in range(chips - 1):
                chip_copy(j, r, piece).wait_recv()
                total = total + chip_in[j, r, piece].astype(F32)
            out_ref[run(r), piece * wide : (piece + 1) * wide] = total.astype(BF16)
    for r in range(2):
        for piece in range(pieces):
            for j in range(chips):
                core_copy(j, r, piece).wait_send()
            for j in range(chips - 1):
                chip_copy(j, r, piece).wait_send()

    def drain(step, carry):
        for g in range(groups):
            for i in range(2):
                kv_copy(g, step, i).wait_send()

                @pl.when(step > 0)
                def _():
                    acc_copy(g, step, i).wait_send()

        return carry

    lax.fori_loop(0, n - 1, drain, 0)
    for g in range(groups):
        for i in range(2):
            acc_copy(g, n - 1, i).wait_send()


def project(grads, weight):
    return lax.dot_general(grads, weight, (((1,), (1,)), ((), ())), preferred_element_type=F32)


def shards(
    n, tp, query_act, key_act, value_act, attn_out, out_grad, log_sum, positions, w_query, w_key, w_value
):
    rows, width = query_act.shape
    dim = HEAD_DIM
    repeat = HEADS // KV_HEADS
    groups = key_act.shape[1] // dim
    heads = groups * repeat
    half = rows // 2
    model = w_query.shape[0]
    cols = model // tp
    chips = tp // 2
    freqs = np.float32(500000.0) ** (-(np.arange(dim // 2, dtype=np.float32) * 2.0 / dim))
    pieces = max(1, cols // PIECE)
    wide = cols // pieces
    vmem = pl.BlockSpec(memory_space=pltpu.VMEM)
    hbm = pl.BlockSpec(memory_space=pl.ANY)
    return pl.pallas_call(
        functools.partial(kernel, n, tp, groups, repeat),
        out_shape=OUT((rows, cols), BF16),
        in_specs=[hbm] * 11,
        out_specs=vmem,
        scratch_shapes=[
            pltpu.VMEM((rows, width), BF16),
            pltpu.VMEM((rows, width), BF16),
            pltpu.VMEM((rows, width), BF16),
            pltpu.VMEM((rows, width), BF16),
            pltpu.VMEM((rows, groups * dim), BF16),
            pltpu.VMEM((rows, groups * dim), BF16),
            pltpu.VMEM(w_query.shape, BF16),
            pltpu.VMEM(w_key.shape, BF16),
            pltpu.VMEM(w_value.shape, BF16),
            pltpu.VMEM((heads, rows), F32),
            pltpu.VMEM((1, rows), jnp.int32),
            pltpu.VMEM((dim // 2, dim), F32),
            pltpu.VMEM((heads, rows), F32),
            pltpu.VMEM((heads, rows), F32),
            pltpu.VMEM((1, rows), F32),
            pltpu.VMEM((dim // 2, rows), F32),
            pltpu.VMEM((dim // 2, rows), F32),
            pltpu.VMEM((tp, 2, pieces, half, wide), F32),
            pltpu.VMEM((chips, 2, pieces, half, wide), BF16),
            pltpu.VMEM((chips, 2, pieces, half, wide), BF16),
            pltpu.VMEM((chips - 1, 2, pieces, half, wide), BF16),
            pltpu.VMEM((chips - 1, 2, pieces, half, wide), BF16),
            pltpu.VMEM((groups, n, 2, 2 * half + 8, dim), BF16),
            pltpu.VMEM((groups, n, 2, 2, half, dim), BF16),
            pltpu.VMEM((groups, n + 1, 2, 2, half, dim), BF16),
            pltpu.VMEM((groups, 2, rows, dim), F32),
            pltpu.VMEM((groups, 2, rows, dim), F32),
            pltpu.VMEM((heads, dim, rows), F32),
            pltpu.SemaphoreType.DMA((groups, 2, n + 1)),
            pltpu.SemaphoreType.DMA((groups, 2, n + 1)),
            pltpu.SemaphoreType.DMA((groups, 2, n + 1)),
            pltpu.SemaphoreType.DMA((groups, 2, n + 1)),
            pltpu.SemaphoreType.DMA((3,)),
            pltpu.SemaphoreType.DMA((3,)),
            pltpu.SemaphoreType.DMA((groups, 2, 2)),
            pltpu.SemaphoreType.DMA((3,)),
            pltpu.SemaphoreType.DMA((chips, 2, pieces)),
            pltpu.SemaphoreType.DMA((chips, 2, pieces)),
            pltpu.SemaphoreType.DMA((chips - 1, 2, pieces)),
            pltpu.SemaphoreType.DMA((chips - 1, 2, pieces)),
        ],
        compiler_params=pltpu.CompilerParams(
            collective_id=0, has_side_effects=True, vmem_limit_bytes=VMEM_LIMIT
        ),
    )(
        query_act,
        out_grad,
        attn_out,
        key_act,
        value_act,
        log_sum,
        positions[None, :],
        jnp.broadcast_to(jnp.asarray(freqs)[:, None], (dim // 2, dim)),
        w_query,
        w_key,
        w_value,
    )


def solution(mesh):
    return jax.shard_map(
        functools.partial(shards, mesh.shape["seq"], mesh.shape["tp"]),
        mesh=mesh,
        in_specs=(
            P("seq", "tp"),
            P("seq", "tp"),
            P("seq", "tp"),
            P("seq", "tp"),
            P("seq", "tp"),
            P("tp", "seq"),
            P("seq"),
            P(None, "tp"),
            P(None, "tp"),
            P(None, "tp"),
        ),
        out_specs=P("seq", "tp"),
        check_vma=False,
    )
```

```python
import functools
import math

import jax
import jax.numpy as jnp
import numpy as np
from jax import lax
from jax.experimental import pallas as pl
from jax.experimental.pallas import tpu as pltpu
from jax.sharding import PartitionSpec as P

HEADS = 32
KV_HEADS = 8
HEAD_DIM = 128
MESH = pl.DeviceIdType.MESH
F32 = jnp.float32
BF16 = jnp.bfloat16
PIECE = 512
VMEM_LIMIT = 58 * 1024 * 1024
OUT = pltpu.VMEM


def ring_place(index, n):
    return jnp.where(index % 2 == 0, index // 2, n - 1 - index // 2)


def ring_index(place, n):
    return jnp.where(place < n // 2, 2 * place, 2 * (n - 1 - place) + 1)


def rotate(grad, cosine, sine):
    half = grad.shape[0] // 2
    first, second = grad[:half], grad[half:]
    return jnp.concatenate([first * cosine + second * sine, second * cosine - first * sine], axis=0)


def kernel(
    n,
    tp,
    groups,
    repeat,
    q_hbm,
    do_hbm,
    o_hbm,
    k_hbm,
    v_hbm,
    log_sum_ref,
    qpos_ref,
    freq_ref,
    wq_hbm,
    wk_hbm,
    wv_hbm,
    out_ref,
    q_ref,
    do_ref,
    o_ref,
    dq_ref,
    dk_ref,
    dv_ref,
    wq_ref,
    wk_ref,
    wv_ref,
    lse_ref,
    delta_ref,
    pos_ref,
    cos_ref,
    sin_ref,
    terms,
    core_out,
    core_in,
    chip_out,
    chip_in,
    kv_buf,
    acc_out,
    acc_in,
    part,
    own,
    dq_acc,
    kv_send,
    kv_recv,
    acc_send,
    acc_recv,
    load_sem,
    in_sem,
    kvin_sem,
    core_send,
    core_recv,
    chip_send,
    chip_recv,
):
    rows, width = q_ref.shape
    half = rows // 2
    dim = width // (groups * repeat)
    scale = dim ** (-0.5)
    log2e = math.log2(math.e)
    place = ring_place(lax.axis_index("seq"), n)
    after = ring_index(lax.rem(place + 1, n), n)
    before = ring_index(lax.rem(place + n - 1, n), n)
    targets = [after if g % 2 == 0 else before for g in range(groups)]

    barrier = pltpu.get_barrier_semaphore()
    for other in (after, before):
        pl.semaphore_signal(barrier, inc=1, device_id={"seq": other}, device_id_type=MESH)
    rank = lax.axis_index("tp")
    chips = tp // 2
    chip, core = rank // 2, lax.rem(rank, 2)
    partner = 2 * chip + 1 - core
    chip_order = [lax.rem(chip + 1 + j, chips) for j in range(chips)]
    peers = [2 * chip_order[j] + core for j in range(chips - 1)]
    for other in [partner] + peers:
        pl.semaphore_signal(barrier, inc=1, device_id={"tp": other}, device_id_type=MESH)

    kv_loads = []
    for g in range(groups):
        cut = pl.ds(g * dim, dim)
        for i, src in enumerate((k_hbm, v_hbm)):
            for r in range(2):
                load = pltpu.make_async_copy(
                    src.at[pl.ds(r * half, half), cut],
                    kv_buf.at[g, 0, r, pl.ds(i * half, half), :],
                    kvin_sem.at[g, i, r],
                )
                load.start()
                kv_loads.append(load)
    in_loads = [
        pltpu.make_async_copy(src, dst, in_sem.at[i])
        for i, (src, dst) in enumerate(((q_hbm, q_ref), (do_hbm, do_ref), (o_hbm, o_ref)))
    ]
    for load in in_loads:
        load.start()
    loads = [
        pltpu.make_async_copy(src, dst, load_sem.at[i])
        for i, (src, dst) in enumerate(((wq_hbm, wq_ref), (wk_hbm, wk_ref), (wv_hbm, wv_ref)))
    ]

    qpos = qpos_ref[...].astype(F32)
    pos_ref[...] = qpos
    for r in range(2):
        tag = jnp.broadcast_to(qpos[:, r * half : r * half + 1] * (1.0 / half), (8, dim)).astype(BF16)
        for g in range(groups):
            kv_buf[g, 0, r, 2 * half : 2 * half + 8, :] = tag

    def kv_copy(g, step, i):
        return pltpu.make_async_remote_copy(
            src_ref=kv_buf.at[g, step, i],
            dst_ref=kv_buf.at[g, step + 1, i],
            send_sem=kv_send.at[g, i, step],
            recv_sem=kv_recv.at[g, i, step + 1],
            device_id={"seq": targets[g]},
            device_id_type=MESH,
        )

    def acc_copy(g, step, i):
        return pltpu.make_async_remote_copy(
            src_ref=acc_out.at[g, step, i],
            dst_ref=acc_in.at[g, step + 1, i],
            send_sem=acc_send.at[g, i, step],
            recv_sem=acc_recv.at[g, i, step + 1],
            device_id={"seq": targets[g]},
            device_id_type=MESH,
        )

    def kv_arrival(g, step, i):
        return pltpu.make_async_remote_copy(
            src_ref=kv_buf.at[g, step, i],
            dst_ref=kv_buf.at[g, step, i],
            send_sem=kv_send.at[g, i, step],
            recv_sem=kv_recv.at[g, i, step],
            device_id={"seq": targets[g]},
            device_id_type=MESH,
        )

    def acc_arrival(g, step, i):
        return pltpu.make_async_remote_copy(
            src_ref=acc_in.at[g, step, i],
            dst_ref=acc_in.at[g, step, i],
            send_sem=acc_send.at[g, i, 0],
            recv_sem=acc_recv.at[g, i, step],
            device_id={"seq": targets[g]},
            device_id_type=MESH,
        )

    for load in kv_loads:
        load.wait()
    pl.semaphore_wait(barrier, 2 + chips)
    for i in range(2):
        for g in range(groups):
            kv_copy(g, 0, i).start()
    for load in loads:
        load.start()

    lse_ref[...] = log_sum_ref[...] * log2e
    for load in in_loads:
        load.wait()
    for h in range(groups * repeat):
        cut = slice(h * dim, (h + 1) * dim)
        both = do_ref[:, cut].astype(F32) * o_ref[:, cut].astype(F32)
        delta_ref[h : h + 1, :] = jnp.sum(both.T, axis=0, keepdims=True)

    angles = freq_ref[:, 0:1] * pos_ref[...]
    cos_ref[...] = jnp.cos(angles)
    sin_ref[...] = jnp.sin(angles)

    def run(r):
        return slice(r * half, (r + 1) * half)

    def attend(g, r, block, result, first):
        k = block[0:half, :]
        v = block[half : 2 * half, :]
        tag = block[2 * half : 2 * half + 8, :].astype(F32)
        low = jnp.concatenate([tag[0:1, :] * half] * (rows // dim), axis=1)
        if first:
            gap = pos_ref[...] - lax.broadcasted_iota(jnp.int32, (half, rows), 0).astype(F32)
            seen = gap >= low
        else:
            hide = jnp.where(pos_ref[...] >= low, 0.0, 1e30)
        kt = k.T
        dk = jnp.zeros((half, dim), F32)
        dv = jnp.zeros((half, dim), F32)
        for c in range(repeat):
            h = g * repeat + c
            q = q_ref[:, h * dim : (h + 1) * dim]
            do = do_ref[:, h * dim : (h + 1) * dim]
            nt = (((1,), (1,)), ((), ()))
            s = lax.dot_general(k, q, nt, preferred_element_type=F32) * (scale * log2e)
            lse = lse_ref[h : h + 1, :]
            if first:
                p = jnp.where(seen, jnp.exp2(s - lse), 0.0)
            else:
                p = jnp.exp2(s - (lse + hide))
            dv += jnp.dot(p.astype(BF16), do, preferred_element_type=F32)
            dp = lax.dot_general(v, do, nt, preferred_element_type=F32)
            ds = (p * (dp - delta_ref[h : h + 1, :])).astype(BF16)
            dk += jnp.dot(ds, q, preferred_element_type=F32)
            dqt = jnp.dot(kt, ds, preferred_element_type=F32)
            if first and r == 0:
                dq_acc[h] = dqt
            else:
                dq_acc[h] += dqt
        result[g, 0, run(r), :] = dk * scale
        result[g, 1, run(r), :] = dv

    for r in range(2):
        for g in range(groups):
            attend(g, r, kv_buf.at[g, 0, r], own, True)

    def take(g, i, step):
        kv_arrival(g, step, i).wait_recv()

        @pl.when(step < n - 1)
        def _():
            kv_copy(g, step, i).start()

    def give(g, i, step):
        @pl.when(step == 1)
        def _():
            acc_out[g, step, i] = part[g, :, run(i), :].astype(BF16)

        @pl.when(step > 1)
        def _():
            acc_arrival(g, step, i).wait_recv()
            total = part[g, :, run(i), :] + acc_in[g, step, i].astype(F32)
            acc_out[g, step, i] = total.astype(BF16)

        acc_copy(g, step, i).start()

    def turn(step, carry):
        for r in range(2):
            for g in range(groups):
                take(g, r, step)
            for g in range(groups):
                attend(g, r, kv_buf.at[g, step, r], part, False)
            for g in range(groups):
                give(g, r, step)
        return carry

    lax.fori_loop(1, n, turn, 0)

    cosine = cos_ref[...]
    sine = sin_ref[...]
    for h in range(groups * repeat):
        dq_ref[:, h * dim : (h + 1) * dim] = rotate(dq_acc[h] * scale, cosine, sine).T.astype(BF16)
    cols = out_ref.shape[1]
    pieces = max(1, cols // PIECE)
    wide = cols // pieces

    def span(block, piece):
        return pl.ds(pl.multiple_of(block * cols + piece * wide, wide), wide)

    for load in loads:
        load.wait()
    far = [2 * chip_order[j] + 1 - core for j in range(chips)]
    near = [2 * chip_order[j] + core for j in range(chips)]

    def query_terms(slot, block, piece):
        both = project(dq_ref[...], wq_ref[span(block, piece), :])
        for r in range(2):
            terms[slot, r, piece] = both[run(r)]

    def finish_grads(r):
        for g in range(groups):
            acc_arrival(g, n, r).wait_recv()
            total = own[g, :, run(r), :] + acc_in[g, n, r].astype(F32)
            cut = slice(g * dim, (g + 1) * dim)
            turned = rotate(total[0].T, cosine[:, run(r)], sine[:, run(r)]).T
            dk_ref[run(r), cut] = turned.astype(BF16)
            dv_ref[run(r), cut] = total[1].astype(BF16)

    def full_terms(slot, block, r, piece):
        total = terms[slot, r, piece] + project(dk_ref[run(r), :], wk_ref[span(block, piece), :])
        return total + project(dv_ref[run(r), :], wv_ref[span(block, piece), :])

    def core_copy(j, r, piece):
        return pltpu.make_async_remote_copy(
            src_ref=core_out.at[j, r, piece],
            dst_ref=core_in.at[j, r, piece],
            send_sem=core_send.at[j, r, piece],
            recv_sem=core_recv.at[j, r, piece],
            device_id={"tp": partner},
            device_id_type=MESH,
        )

    def chip_copy(j, r, piece):
        return pltpu.make_async_remote_copy(
            src_ref=chip_out.at[j, r, piece],
            dst_ref=chip_in.at[j, r, piece],
            send_sem=chip_send.at[j, r, piece],
            recv_sem=chip_recv.at[j, r, piece],
            device_id={"tp": peers[j]},
            device_id_type=MESH,
        )

    def relay(j, r, piece):
        core_copy(j, r, piece).wait_recv()
        mine = terms[2 * j + 1, r, piece] + core_in[j, r, piece].astype(F32)
        if j < chips - 1:
            chip_out[j, r, piece] = mine.astype(BF16)
            chip_copy(j, r, piece).start()
        else:
            terms[2 * j + 1, r, piece] = mine

    def share(j, r):
        for piece in range(pieces):
            if r == 0:
                query_terms(2 * j, far[j], piece)
            core_out[j, r, piece] = full_terms(2 * j, far[j], r, piece).astype(BF16)
            core_copy(j, r, piece).start()
        for piece in range(pieces):
            if r == 0:
                query_terms(2 * j + 1, near[j], piece)
            terms[2 * j + 1, r, piece] = full_terms(2 * j + 1, near[j], r, piece)
            relay(j, r, piece)

    for r in range(2):
        finish_grads(r)
        for j in range(chips - 1):
            share(j, r)
    for r in range(2):
        share(chips - 1, r)

    for r in range(2):
        for piece in range(pieces):
            total = terms[2 * chips - 1, r, piece]
            for j in range(chips - 1):
                chip_copy(j, r, piece).wait_recv()
                total = total + chip_in[j, r, piece].astype(F32)
            out_ref[run(r), piece * wide : (piece + 1) * wide] = total.astype(BF16)
    for r in range(2):
        for piece in range(pieces):
            for j in range(chips):
                core_copy(j, r, piece).wait_send()
            for j in range(chips - 1):
                chip_copy(j, r, piece).wait_send()

    def drain(step, carry):
        for g in range(groups):
            for i in range(2):
                kv_copy(g, step, i).wait_send()

                @pl.when(step > 0)
                def _():
                    acc_copy(g, step, i).wait_send()

        return carry

    lax.fori_loop(0, n - 1, drain, 0)
    for g in range(groups):
        for i in range(2):
            acc_copy(g, n - 1, i).wait_send()


def project(grads, weight):
    return lax.dot_general(grads, weight, (((1,), (1,)), ((), ())), preferred_element_type=F32)


def shards(
    n, tp, query_act, key_act, value_act, attn_out, out_grad, log_sum, positions, w_query, w_key, w_value
):
    rows, width = query_act.shape
    dim = HEAD_DIM
    repeat = HEADS // KV_HEADS
    groups = key_act.shape[1] // dim
    heads = groups * repeat
    half = rows // 2
    model = w_query.shape[0]
    cols = model // tp
    chips = tp // 2
    freqs = np.float32(500000.0) ** (-(np.arange(dim // 2, dtype=np.float32) * 2.0 / dim))
    pieces = max(1, cols // PIECE)
    wide = cols // pieces
    vmem = pl.BlockSpec(memory_space=pltpu.VMEM)
    hbm = pl.BlockSpec(memory_space=pl.ANY)
    return pl.pallas_call(
        functools.partial(kernel, n, tp, groups, repeat),
        out_shape=OUT((rows, cols), BF16),
        in_specs=[hbm] * 5 + [vmem] * 3 + [hbm] * 3,
        out_specs=vmem,
        scratch_shapes=[
            pltpu.VMEM((rows, width), BF16),
            pltpu.VMEM((rows, width), BF16),
            pltpu.VMEM((rows, width), BF16),
            pltpu.VMEM((rows, width), BF16),
            pltpu.VMEM((rows, groups * dim), BF16),
            pltpu.VMEM((rows, groups * dim), BF16),
            pltpu.VMEM(w_query.shape, BF16),
            pltpu.VMEM(w_key.shape, BF16),
            pltpu.VMEM(w_value.shape, BF16),
            pltpu.VMEM((heads, rows), F32),
            pltpu.VMEM((heads, rows), F32),
            pltpu.VMEM((1, rows), F32),
            pltpu.VMEM((dim // 2, rows), F32),
            pltpu.VMEM((dim // 2, rows), F32),
            pltpu.VMEM((tp, 2, pieces, half, wide), F32),
            pltpu.VMEM((chips, 2, pieces, half, wide), BF16),
            pltpu.VMEM((chips, 2, pieces, half, wide), BF16),
            pltpu.VMEM((chips - 1, 2, pieces, half, wide), BF16),
            pltpu.VMEM((chips - 1, 2, pieces, half, wide), BF16),
            pltpu.VMEM((groups, n, 2, 2 * half + 8, dim), BF16),
            pltpu.VMEM((groups, n, 2, 2, half, dim), BF16),
            pltpu.VMEM((groups, n + 1, 2, 2, half, dim), BF16),
            pltpu.VMEM((groups, 2, rows, dim), F32),
            pltpu.VMEM((groups, 2, rows, dim), F32),
            pltpu.VMEM((heads, dim, rows), F32),
            pltpu.SemaphoreType.DMA((groups, 2, n + 1)),
            pltpu.SemaphoreType.DMA((groups, 2, n + 1)),
            pltpu.SemaphoreType.DMA((groups, 2, n + 1)),
            pltpu.SemaphoreType.DMA((groups, 2, n + 1)),
            pltpu.SemaphoreType.DMA((3,)),
            pltpu.SemaphoreType.DMA((3,)),
            pltpu.SemaphoreType.DMA((groups, 2, 2)),
            pltpu.SemaphoreType.DMA((chips, 2, pieces)),
            pltpu.SemaphoreType.DMA((chips, 2, pieces)),
            pltpu.SemaphoreType.DMA((chips - 1, 2, pieces)),
            pltpu.SemaphoreType.DMA((chips - 1, 2, pieces)),
        ],
        compiler_params=pltpu.CompilerParams(
            collective_id=0, has_side_effects=True, vmem_limit_bytes=VMEM_LIMIT
        ),
    )(
        query_act,
        out_grad,
        attn_out,
        key_act,
        value_act,
        log_sum,
        positions[None, :],
        jnp.broadcast_to(jnp.asarray(freqs)[:, None], (dim // 2, dim)),
        w_query,
        w_key,
        w_value,
    )


def solution(mesh):
    return jax.shard_map(
        functools.partial(shards, mesh.shape["seq"], mesh.shape["tp"]),
        mesh=mesh,
        in_specs=(
            P("seq", "tp"),
            P("seq", "tp"),
            P("seq", "tp"),
            P("seq", "tp"),
            P("seq", "tp"),
            P("tp", "seq"),
            P("seq"),
            P(None, "tp"),
            P(None, "tp"),
            P(None, "tp"),
        ),
        out_specs=P("seq", "tp"),
        check_vma=False,
    )
```
